32 devices in a mesh: gx: 8 (over y, x, core), gy: 4 (over z).
Axes of the slice: x: 2, y: 2, z: 4, core: 2. Of those that a mesh axis runs over, the one named last changes fastest.
Arguments:
- u_old: float32 [3, 256, 128, 256], P(None, 'gx', 'gy'), may hold values from -0.6 to 0.6
- density: float32 [256, 128, 256], P('gx', 'gy'), may hold values from 0.5 to 2
- offsets: float32 [3, 512, 128], P(None, ('gx', 'gy')), may hold values from 0 to 1
- forces: float32 [3, 512, 128], P(None, ('gx', 'gy')), may hold values from -60 to 60
- base_x: int32 [512, 128], P(('gx', 'gy')), may hold values from 0 to 31
- base_y: int32 [512, 128], P(('gx', 'gy')), may hold values from 0 to 31
- base_z: int32 [512, 128], P(('gx', 'gy')), may hold values from 0 to 255
- tile_count: int32 [32], P(('gx', 'gy')), may hold values from 1 to 16, as said below
Outputs:
- u_new: float32 [3, 256, 128, 256], P(None, 'gx', 'gy')
- marker_velocity: float32 [3, 512, 128], P(None, ('gx', 'gy'))
The draws below stay inside these ranges and needn't reach their ends.
Inputs may be any that keep to these rules, and one draw needn't show every extreme that they name: `tile_count`: every draw has a device with exactly 16 live tiles; loads are skewed, with a mean near a quarter of that.
All inputs are finite; a program needn't handle non-finite values.
Results may differ from the reference program's by a relative error of at most 0.000075.
Values sent between devices are 32-bit elements; how exact they have to be, the bound alone decides.
A program may use at most 64 MiB of HBM per device.

```python
import math
import jax
import jax.numpy as jnp

CX = 32
CY = 32
NZ = 256
TILE = 128
MAXT = 16
NX = 256
NY = 128
TILES = 512
N_GY = 4
DEVICES = 32


def draw_tile_count(key, part):
    first, second, third = jax.random.split(jax.random.fold_in(key, 17), 3)
    upper = jax.random.randint(first, (DEVICES,), 0, MAXT)
    lower = jax.random.randint(second, (DEVICES,), 0, MAXT)
    counts = 1 + upper * lower // MAXT
    busiest = jax.random.randint(third, (), 0, DEVICES)
    return jnp.where(jnp.arange(DEVICES) == busiest, MAXT, counts).astype(jnp.int32)


def plant(drawn, key, least, top_value):
    index_at = [jax.random.randint(jax.random.fold_in(key, axis), (), 0, length) for axis, length in enumerate(drawn.shape)]
    widest = drawn.shape.index(max(drawn.shape))
    next_to = index_at[:widest] + [(index_at[widest] + 1) % drawn.shape[widest]] + index_at[widest + 1:]
    return drawn.at[tuple(index_at)].set(least).at[tuple(next_to)].set(top_value)


def block_levels(stream_key, dims, shards, least, largest):
    level, own = 1.0, jax.random.fold_in(stream_key, 6)
    for dim, shards_of in shards:
        steps = jnp.exp(jax.random.uniform(jax.random.fold_in(own, dim), (shards_of,), jnp.float32, least / len(shards), largest / len(shards)))
        level = level * jnp.repeat(steps, dims[dim] // shards_of).reshape([-1 if axis == dim else 1 for axis in range(len(dims))])
    return level


def noise(own_key, dims, scale, most, cuts=(), kind=jnp.bfloat16):
    drawn = jax.random.normal(own_key, dims, jnp.float32) * scale
    if len(cuts) > 0:
        drawn = block_levels(own_key, dims, cuts, -0.22, 0.18) * drawn
    return jnp.clip(drawn, min=-most, max=most).astype(kind)


def setup_inputs(seed: int = 0) -> dict:
    key_list = jax.random.split(jax.random.key(seed), 9)
    return {
        "u_old": noise(key_list[0], (3, NX, NY, NZ), 0.1, 0.6, ((1, 8), (2, 4)), jnp.float32),
        "density": jnp.clip(jnp.exp(math.log(2.0) - 1.3862944 * jax.random.uniform(key_list[1], (NX, NY, NZ), jnp.float32) ** block_levels(key_list[1], (NX, NY, NZ), ((0, 8), (1, 4)), -0.2, 0.2)), 0.5, 2.0),
        "offsets": jnp.clip(1.0 * jax.random.uniform(key_list[2], (3, TILES, TILE), jnp.float32) ** block_levels(key_list[2], (3, TILES, TILE), ((1, 32),), -0.2, 0.2), 0.0, 1.0),
        "forces": noise(key_list[3], (3, TILES, TILE), 10.0, 60.0, ((1, 32),), jnp.float32),
        "base_x": plant(jax.random.randint(key_list[4], (TILES, TILE), 0, CX), jax.random.fold_in(key_list[4], 1), 0, CX - 1).astype(jnp.int32),
        "base_y": plant(jax.random.randint(key_list[5], (TILES, TILE), 0, CY), jax.random.fold_in(key_list[5], 1), 0, CY - 1).astype(jnp.int32),
        "base_z": plant(jax.random.randint(key_list[6], (TILES, TILE), 0, NZ), jax.random.fold_in(key_list[6], 1), 0, NZ - 1).astype(jnp.int32),
        "tile_count": draw_tile_count(jax.random.fold_in(key_list[8], 71), 0),
    }


def stencil(frac):
    root = jnp.sqrt(1.0 + 4.0 * frac - 4.0 * frac * frac)
    return [(3.0 - 2.0 * frac - root) / 8.0, (3.0 - 2.0 * frac + root) / 8.0, (1.0 + 2.0 * frac + root) / 8.0, (1.0 + 2.0 * frac - root) / 8.0]

def reference(u_old, density, offsets, forces, base_x, base_y, base_z, tile_count):
    time_step = 0.5
    tiles, width = base_x.shape
    nx, ny, nz = density.shape
    slot = jnp.arange(tiles).astype(jnp.int32)
    device = slot // MAXT
    anchor_x = (device // N_GY * CX)[:, None]
    anchor_y = (device % N_GY * CY)[:, None]
    live = (slot % MAXT < tile_count[device]).astype(jnp.float32)[:, None] * jnp.ones((tiles, width), jnp.float32)
    weight_x = stencil(offsets[0])
    weight_y = stencil(offsets[1])
    weight_z = stencil(offsets[2])
    load = forces * live[None]
    grid = jnp.zeros((3, nx * ny * nz), jnp.float32)
    places = []
    for shift_a in range(4):
        cell_x = (anchor_x + base_x + shift_a - 1) % nx
        for shift_b in range(4):
            cell_y = (anchor_y + base_y + shift_b - 1) % ny
            for shift_c in range(4):
                cell_z = (base_z + shift_c - 1) % nz
                index = ((cell_x * ny + cell_y) * nz + cell_z).astype(jnp.int32)
                weight = weight_x[shift_a] * weight_y[shift_b] * weight_z[shift_c]
                grid = grid.at[:, index.reshape(-1)].add((load * weight[None]).reshape(3, -1))
                places.append((index, weight))
    force_grid = grid.reshape(3, nx, ny, nz)
    u_new = u_old + time_step * force_grid / density[None]
    table = u_new.reshape(3, -1)
    velocity = jnp.zeros((3, tiles, width), jnp.float32)
    for index, weight in places:
        velocity = velocity + table[:, index.reshape(-1)].reshape(3, tiles, width) * weight[None]
    return (u_new, velocity * live[None])
```

```python
import functools

import jax
import jax.numpy as jnp
from jax import lax
from jax.experimental import pallas as pl
from jax.experimental.pallas import tpu as pltpu
from jax.sharding import PartitionSpec as P

VMEM_LIMIT = 60 * 1024 * 1024


def divisor(count, most):
    return max(d for d in range(1, most + 1) if count % d == 0)


def moved(value, step_x, step_y):
    if step_y == 0:
        n = lax.axis_size("gx")
        return lax.ppermute(value, "gx", [(i, (i + step_x) % n) for i in range(n)])
    if step_x == 0:
        n = lax.axis_size("gy")
        return lax.ppermute(value, "gy", [(i, (i + step_y) % n) for i in range(n)])
    nx, ny = lax.axis_size("gx"), lax.axis_size("gy")
    pairs = [
        (i * ny + j, ((i + step_x) % nx) * ny + (j + step_y) % ny)
        for i in range(nx)
        for j in range(ny)
    ]
    return lax.ppermute(value, ("gx", "gy"), pairs)


def stencil(frac):
    root = jnp.sqrt(1.0 + 4.0 * frac - 4.0 * frac * frac)
    return [
        (3.0 - 2.0 * frac - root) / 8.0,
        (3.0 - 2.0 * frac + root) / 8.0,
        (1.0 + 2.0 * frac + root) / 8.0,
        (1.0 + 2.0 * frac - root) / 8.0,
    ]


def pick(delta, four):
    total = jnp.where(delta == 0, four[0], 0.0)
    for k in range(1, 4):
        total = jnp.where(delta == k, four[k], total)
    return total


def wrapped(delta, length):
    delta = jnp.where(delta < 0, delta + length, delta)
    return jnp.where(delta >= length, delta - length, delta)


def edge_weights(frac, base, rows, size):
    row = lax.broadcasted_iota(jnp.int32, (rows, base.shape[1]), 0)
    cell = jnp.where(row == size + 2, -1, row)
    cell = jnp.where(row > size + 2, -8, cell)
    return pick(cell - base + 1, stencil(frac))


def halves(value):
    high = value.astype(jnp.bfloat16)
    low = (value - high.astype(jnp.float32)).astype(jnp.bfloat16)
    return high, low


def edges(size):
    return (size - 1, size, size + 1), (size + 2, 0, 1)


def spread_kernel(size_x, size_y, feat, base, grid, *refs):
    slabs, (wx_s, wy_s, high_s, low_s) = refs[:8], refs[8:]
    planes, rows, depth = grid.shape[1], grid.shape[2], grid.shape[3]
    markers = feat.shape[1]
    wx_s[...] = edge_weights(feat[0:1, :], base[0:1, :], wx_s.shape[0], size_x)
    wy_s[...] = edge_weights(feat[1:2, :], base[1:2, :], rows, size_y)
    four = stencil(feat[2:3, :])
    column = jnp.concatenate(
        four + [base[2:3, :].astype(jnp.float32)] + [feat[3 + c : 4 + c, :] for c in range(3)], axis=0
    ).T
    cut = 256 if markers % 256 == 0 else 128
    for start in range(0, markers, cut):
        part = column[start : start + cut]
        lane = lax.broadcasted_iota(jnp.int32, (cut, depth), 1)
        delta = wrapped(lane - part[:, 4:5].astype(jnp.int32) + 1, depth)
        wz = pick(delta, [part[:, k : k + 1] for k in range(4)])
        for c in range(3):
            high, low = halves(wz * part[:, 5 + c : 6 + c])
            high_s[start : start + cut, c * depth : (c + 1) * depth] = high
            low_s[start : start + cut, c * depth : (c + 1) * depth] = low
    group = divisor(planes, 8)

    def turn(g, carry):
        first = g * group
        left = jnp.concatenate(
            [wy_s[...] * wx_s[pl.ds(first + j, 1), :] for j in range(group)], axis=0
        )
        high, low = halves(left)
        dot = functools.partial(jnp.dot, preferred_element_type=jnp.float32)
        total = dot(high, high_s[...]) + dot(low, high_s[...]) + dot(high, low_s[...])
        for j in range(group):
            for c in range(3):
                grid[c, first + j] = total[j * rows : (j + 1) * rows, c * depth : (c + 1) * depth]
        return carry

    lax.fori_loop(0, planes // group, turn, 0)
    sides_x, sides_y = edges(size_x), edges(size_y)
    for side in range(2):
        for c in range(3):
            for j, p in enumerate(sides_x[side]):
                slabs[side][c, j] = grid[c, p]
                for other in range(2):
                    for i, r in enumerate(sides_y[other]):
                        slabs[4 + 2 * side + other][c, j, i : i + 1] = grid[c, p, r : r + 1]
            for i, r in enumerate(sides_y[side]):
                for p in range(planes):
                    slabs[2 + side][c, i, p : p + 1] = grid[c, p, r : r + 1]


def read_kernel(size_x, size_y, time_step, *refs):
    feat, base, grid, u_old, density, low_x, high_x, low_y, high_y = refs[:9]
    slabs, (u_new, velocity) = refs[9:17], refs[17:19]
    total, wx_s, wy_s, wz3, table = refs[19:]
    planes, rows, depth = grid.shape[1], grid.shape[2], grid.shape[3]
    markers = feat.shape[1]
    wx_s[...] = edge_weights(feat[0:1, :], base[0:1, :], wx_s.shape[0], size_x)
    wy_s[...] = edge_weights(feat[1:2, :], base[1:2, :], rows, size_y)
    cut = 256 if markers % 256 == 0 else 128
    for start in range(0, markers, cut):
        at = slice(start, start + cut)
        row = lax.broadcasted_iota(jnp.int32, (depth, cut), 0)
        delta = wrapped(row - base[2:3, at] + 1, depth)
        high, low = halves(pick(delta, stencil(feat[2:3, at])))
        wz3[0:depth, at] = high
        wz3[depth : 2 * depth, at] = high
        wz3[2 * depth :, at] = low
    total[...] = grid[...]
    near_x, near_y = edges(size_x)[::-1], edges(size_y)[::-1]
    for side in range(2):
        for c in range(3):
            for j, p in enumerate(near_x[side]):
                total[c, p] = total[c, p] + slabs[side][c, j]
                for other in range(2):
                    for i, r in enumerate(near_y[other]):
                        total[c, p, r : r + 1] = (
                            total[c, p, r : r + 1] + slabs[4 + 2 * side + other][c, j, i : i + 1]
                        )
            for i, r in enumerate(near_y[side]):
                for p in range(planes):
                    total[c, p, r : r + 1] = total[c, p, r : r + 1] + slabs[2 + side][c, i, p : p + 1]
    group = divisor(planes, 6)
    spare = jnp.ones((rows - size_y - 3, depth), jnp.float32)

    def plane_state(k, p):
        if p < size_x:
            main = density[p] if k == 3 else u_old[k, p]
        elif p < size_x + 2:
            main = high_x[k, p - size_x]
        else:
            main = low_x[k, 0]
        edge = [high_y[k, 0, p : p + 1], high_y[k, 1, p : p + 1], low_y[k, 0, p : p + 1], spare]
        return jnp.concatenate([main] + edge, axis=0)

    for g in range(planes // group):
        pieces = []
        for p in range(g * group, (g + 1) * group):
            scale = time_step / plane_state(3, p)
            for c in range(3):
                value = plane_state(c, p) + total[c, p] * scale
                if p < size_x:
                    u_new[c, p] = value[:size_y]
                pieces.append(value)
        high, low = halves(jnp.concatenate(pieces, axis=0))
        table[g, :, 0:depth] = high
        table[g, :, depth : 2 * depth] = low
        table[g, :, 2 * depth :] = high

    def turn(step, carry):
        at = pl.ds(pl.multiple_of(step * cut, cut), cut)
        right = wz3[:, at]
        wy = wy_s[:, at]
        sums = [jnp.zeros((8, cut), jnp.float32) for _ in range(3)]
        for g in range(planes // group):
            found = jnp.dot(table[g], right, preferred_element_type=jnp.float32)
            for j in range(group):
                p = g * group + j
                weight = wy * wx_s[p : p + 1, at]
                for c in range(3):
                    first = (j * 3 + c) * rows
                    product = found[first : first + rows] * weight
                    for r in range(0, rows, 8):
                        sums[c] = sums[c] + product[r : r + 8]
        velocity[:, at] = (
            jnp.concatenate([jnp.sum(s, axis=0, keepdims=True) for s in sums], axis=0) * feat[6:7, at]
        )
        return carry

    lax.fori_loop(0, markers // cut, turn, 0)


def on_device(u_old, density, offsets, forces, base_x, base_y, base_z, tile_count):
    time_step = 0.5
    _, size_x, size_y, depth = u_old.shape
    slots, width = base_x.shape
    markers = slots * width
    planes = size_x + 3
    rows = -(-(size_y + 3) // 8) * 8
    lines = -(-planes // 8) * 8
    f32, bf16 = jnp.float32, jnp.bfloat16
    live = (lax.broadcasted_iota(jnp.int32, (slots, width), 0) < tile_count[0]).astype(f32)
    feat = jnp.concatenate([offsets, forces * live[None], live[None]], axis=0).reshape(7, markers)
    base = jnp.stack([base_x, base_y, base_z], axis=0).reshape(3, markers)

    up = jnp.concatenate([u_old[:, size_x - 1 :], density[None, size_x - 1 :]], axis=0)
    down = jnp.concatenate([u_old[:, :2], density[None, :2]], axis=0)
    low_x, high_x = moved(up, 1, 0), moved(down, -1, 0)

    def strip(r):
        inner = jnp.concatenate([u_old[:, :, r], density[None, :, r]], axis=0)
        return jnp.concatenate([inner, high_x[:, :, r], low_x[:, :, r]], axis=1)

    low_y = moved(strip(size_y - 1)[:, None], 0, 1)
    high_y = moved(jnp.stack([strip(0), strip(1)], axis=1), 0, -1)

    params = pltpu.CompilerParams(vmem_limit_bytes=VMEM_LIMIT)
    slab_x = jax.ShapeDtypeStruct((3, 3, rows, depth), f32)
    slab_y = jax.ShapeDtypeStruct((3, 3, planes, depth), f32)
    corner = jax.ShapeDtypeStruct((3, 3, 3, depth), f32)
    whole = pl.BlockSpec(memory_space=pltpu.VMEM)
    flops = 6 * planes * rows * 3 * depth * markers
    cost = pl.CostEstimate(flops=flops, transcendentals=0, bytes_accessed=8 * planes * rows * depth)
    grid, *slabs = pl.pallas_call(
        functools.partial(spread_kernel, size_x, size_y),
        out_shape=[jax.ShapeDtypeStruct((3, planes, rows, depth), f32)]
        + [slab_x] * 2
        + [slab_y] * 2
        + [corner] * 4,
        in_specs=[whole] * 2,
        out_specs=[whole] * 9,
        scratch_shapes=[
            pltpu.VMEM((lines, markers), f32),
            pltpu.VMEM((rows, markers), f32),
            pltpu.VMEM((markers, 3 * depth), bf16),
            pltpu.VMEM((markers, 3 * depth), bf16),
        ],
        compiler_params=params,
        cost_estimate=cost,
        name="spread",
    )(feat, base)
    ways = [(1, 0), (-1, 0), (0, 1), (0, -1), (1, 1), (1, -1), (-1, 1), (-1, -1)]
    slabs = [moved(slab, *way) for slab, way in zip(slabs, ways)]
    group = divisor(planes, 6)
    u_new, velocity = pl.pallas_call(
        functools.partial(read_kernel, size_x, size_y, time_step),
        out_shape=[
            jax.ShapeDtypeStruct(u_old.shape, f32),
            jax.ShapeDtypeStruct((3, markers), f32),
        ],
        in_specs=[whole] * 17,
        out_specs=[whole] * 2,
        scratch_shapes=[
            pltpu.VMEM((3, planes, rows, depth), f32),
            pltpu.VMEM((lines, markers), f32),
            pltpu.VMEM((rows, markers), f32),
            pltpu.VMEM((3 * depth, markers), bf16),
            pltpu.VMEM((planes // group, group * 3 * rows, 3 * depth), bf16),
        ],
        compiler_params=params,
        cost_estimate=cost,
        name="read",
    )(feat, base, grid, u_old, density, low_x, high_x, low_y, high_y, *slabs)
    return (u_new, velocity.reshape(3, slots, width))


def solution(mesh):
    in_specs = (
        P(None, "gx", "gy", None),
        P("gx", "gy", None),
        P(None, ("gx", "gy"), None),
        P(None, ("gx", "gy"), None),
        P(("gx", "gy"), None),
        P(("gx", "gy"), None),
        P(("gx", "gy"), None),
        P(("gx", "gy")),
    )
    out_specs = (P(None, "gx", "gy", None), P(None, ("gx", "gy"), None))
    return jax.shard_map(
        on_device, mesh=mesh, in_specs=in_specs, out_specs=out_specs, check_vma=False
    )
```
